32 devices in a mesh: gx: 8 (over z, core), gy: 4 (over y, x).
Axes of the slice: x: 2, y: 2, z: 4, core: 2. Of those that a mesh axis runs over, the one named last changes fastest.
Arguments:
- density: float32 [256, 256, 256], P('gx', 'gy'), may hold values from 0.05 to 2
Outputs:
- potential: float32 [256, 256, 256], P('gx', 'gy')
- energy: float32 [], replicated
The draws below stay inside these ranges and needn't reach their ends.
All inputs are finite; a program needn't handle non-finite values.
Results may differ from the reference program's by a relative error of at most 0.00005.
Values sent between devices are 32-bit elements.
A program may use at most 128 MiB of HBM per device.

```python
import math
import jax
import jax.numpy as jnp

NX = 256
NY = 256
NZ = 256


def block_scale(stream_key, dims, split, least, high):
    gain = 1.0
    for position, blocks in split:
        heights = jax.random.uniform(jax.random.fold_in(jax.random.fold_in(stream_key, 6), position), (blocks,), jnp.float32, least / len(split), high / len(split))
        gain = gain * jnp.repeat(jnp.exp(heights), dims[position] // blocks).reshape((-1,) + (1,) * (len(dims) - 1 - position))
    return gain


def setup_inputs(seed: int = 0) -> dict:
    streams_of = jax.random.split(jax.random.key(seed), 2)
    density = jnp.clip(jnp.exp(math.log(2.0) - 3.6888794 * jax.random.uniform(streams_of[0], (NX, NY, NZ), jnp.float32) ** block_scale(streams_of[0], (NX, NY, NZ), ((0, 8), (1, 4)), -0.2, 0.2)), 0.05, 2.0)
    return dict(density=density)


spacing = 1.0
pbe_kappa = 0.804
pbe_mu = 0.2195149727645171
pbe_beta = 0.06672455060314922
pbe_gamma = 0.031090690869654894
pw_coef = 0.0310907
pw_alpha = 0.2137
pw_first = 7.5957
pw_second = 3.5876
pw_third = 1.6382
pw_fourth = 0.49294

def xc_energy(electrons, grad_sq):
    k_fermi = jnp.cbrt(3.0 * math.pi ** 2 * electrons)
    exch_unif = -0.75 * k_fermi / math.pi
    s_square = grad_sq / (4.0 * k_fermi ** 2 * electrons ** 2)
    enhance = 1.0 + pbe_kappa - pbe_kappa / (1.0 + pbe_mu * s_square / pbe_kappa)
    wigner = jnp.cbrt(3.0 / (4.0 * math.pi * electrons))
    root_rs = jnp.sqrt(wigner)
    series = 2.0 * pw_coef * (pw_first * root_rs + pw_second * wigner + pw_third * wigner * root_rs + pw_fourth * wigner ** 2)
    corr_unif = -2.0 * pw_coef * (1.0 + pw_alpha * wigner) * jnp.log(1.0 + 1.0 / series)
    screen_sq = 4.0 * k_fermi / math.pi
    t_square = grad_sq / (4.0 * screen_sq * electrons ** 2)
    factor = pbe_beta / pbe_gamma / jnp.expm1(-corr_unif / pbe_gamma)
    scaled = factor * t_square
    gradient_term = pbe_gamma * jnp.log(1.0 + pbe_beta / pbe_gamma * t_square * (1.0 + scaled) / (1.0 + scaled + scaled ** 2))
    return electrons * (exch_unif * enhance + corr_unif + gradient_term)

def summed_energy(electrons, grad_sq):
    return jnp.sum(xc_energy(electrons, grad_sq))

def wavenum(count):
    index = jnp.arange(count, dtype=jnp.int32)
    signed = jnp.where(index < count // 2, index, index - count)
    signed = jnp.where(index == count // 2, 0, signed)
    return signed.astype(jnp.float32) * (2.0 * math.pi / (count * spacing))

def reference(density):
    spectrum = jnp.fft.fftn(density)
    waves = (wavenum(NX)[:, None, None], wavenum(NY)[None, :, None], wavenum(NZ)[None, None, :])
    gradients = [jnp.real(jnp.fft.ifftn(1j * wavevec * spectrum)) for wavevec in waves]
    grad_sq = gradients[0] ** 2 + gradients[1] ** 2 + gradients[2] ** 2
    energy_sum, partials = jax.value_and_grad(summed_energy, argnums=(0, 1))(density, grad_sq)
    d_dens, d_grad = partials
    flux_spec = 1j * waves[0] * jnp.fft.fftn(2.0 * d_grad * gradients[0])
    flux_spec = flux_spec + 1j * waves[1] * jnp.fft.fftn(2.0 * d_grad * gradients[1])
    flux_spec = flux_spec + 1j * waves[2] * jnp.fft.fftn(2.0 * d_grad * gradients[2])
    divergence = jnp.real(jnp.fft.ifftn(flux_spec))
    potential = d_dens - divergence
    energy = energy_sum / (NX * NY * NZ)
    return (potential, energy)
```

```python
import functools
import math

import jax
import jax.numpy as jnp
import numpy as np
from jax import lax
from jax.experimental import pallas as pl
from jax.experimental.pallas import tpu as pltpu
from jax.sharding import PartitionSpec as P

spacing = 1.0
highest = lax.Precision.HIGHEST
pbe_kappa = 0.804
pbe_mu = 0.2195149727645171
pbe_beta = 0.06672455060314922
pbe_gamma = 0.031090690869654894
pw_coef = 0.0310907
pw_alpha = 0.2137
pw_first = 7.5957
pw_second = 3.5876
pw_third = 1.6382
pw_fourth = 0.49294


def xc_energy(electrons, grad_sq):
    third = jnp.exp(jnp.log(electrons) * (1.0 / 3.0))
    k_fermi = (3.0 * math.pi**2) ** (1.0 / 3.0) * third
    exch_unif = -0.75 / math.pi * k_fermi
    inv_sq = grad_sq / (4.0 * k_fermi * electrons * electrons)
    s_square = inv_sq / k_fermi
    enhance = 1.0 + pbe_kappa - pbe_kappa / (1.0 + (pbe_mu / pbe_kappa) * s_square)
    wigner = (3.0 / (4.0 * math.pi)) ** (1.0 / 3.0) / third
    root_rs = jnp.sqrt(wigner)
    series = (
        2.0
        * pw_coef
        * root_rs
        * (pw_first + root_rs * (pw_second + root_rs * (pw_third + root_rs * pw_fourth)))
    )
    corr_unif = -2.0 * pw_coef * (1.0 + pw_alpha * wigner) * jnp.log(1.0 + 1.0 / series)
    t_square = inv_sq * (math.pi / 4.0)
    factor = (pbe_beta / pbe_gamma) / (jnp.exp(corr_unif * (-1.0 / pbe_gamma)) - 1.0)
    scaled = factor * t_square
    gradient_term = pbe_gamma * jnp.log(
        1.0 + (pbe_beta / pbe_gamma) * t_square * (1.0 + scaled) / (1.0 + scaled + scaled * scaled)
    )
    return electrons * (exch_unif * enhance + corr_unif + gradient_term)


def deriv_matrix(count):
    positions = np.arange(count)
    signed = np.where(positions < count // 2, positions, positions - count)
    signed = np.where(positions == count // 2, 0, signed)
    waves = signed * (2.0 * math.pi / (count * spacing))
    phase = (positions[:, None] * positions[None, :] % count) * (2.0 * math.pi / count)
    cosine, sine = np.cos(phase), np.sin(phase)
    first = (cosine.T * waves[None, :]) @ sine
    second = (sine.T * waves[None, :]) @ cosine
    return ((first - second) / count).astype(np.float32)


def far_first(count):
    return sorted(range(1, count), key=lambda k: abs(2 * k - count))


def kernel(
    num_gx, num_gy, zc,
    n_ref, dmx_ref, dmy_ref, dmz_ref,
    out_ref, energy_ref,
    n_t, lx1, rx1, gx_t, gx, ly1, ry1, gy, gz, fx_t, lx2, rx2, dx_t, ly2, ry2, dy,
    acc, part_y, tot_y, part_x,
    xs_sem, xr_sem, ys_sem, yr_sem, es_sem, er_sem,
):
    rows_x, rows_y, count_z = n_ref.shape
    block_y = rows_y // num_gx
    block_x = rows_x // num_gy
    count_x = rows_x * num_gx
    count_y = rows_y * num_gy
    chunks = count_z // zc
    me_x = lax.axis_index("gx")
    me_y = lax.axis_index("gy")

    def peer_x(k):
        return lax.rem(me_x + k, num_gx)

    def peer_y(k):
        return lax.rem(me_y + k, num_gy)

    def zs(c):
        return pl.ds(c * zc, zc)

    def x_block(i):
        return pl.ds(i * block_y, block_y)

    def x_rows(i):
        return pl.ds(pl.multiple_of(i * rows_x, rows_x), rows_x)

    def y_block(i):
        return pl.ds(i * block_x, block_x)

    def y_rows(i):
        return pl.ds(pl.multiple_of(i * rows_y, rows_y), rows_y)

    barrier = pltpu.get_barrier_semaphore()
    for k in range(1, num_gx):
        pl.semaphore_signal(
            barrier, inc=1, device_id={"gx": peer_x(k)}, device_id_type=pl.DeviceIdType.MESH
        )
    for k in range(1, num_gy):
        pl.semaphore_signal(
            barrier, inc=1, device_id={"gy": peer_y(k)}, device_id_type=pl.DeviceIdType.MESH
        )
    pl.semaphore_wait(barrier, num_gx + num_gy - 2)

    def send_x(phase, c, source, target, forward):
        copies = []
        for k in far_first(num_gx):
            to = peer_x(k)
            if forward:
                src, dst = source.at[x_block(to), :, zs(c)], target.at[:, x_rows(me_x), zs(c)]
            else:
                src, dst = source.at[:, x_rows(to), zs(c)], target.at[x_block(me_x), :, zs(c)]
            copy = pltpu.make_async_remote_copy(
                src_ref=src, dst_ref=dst,
                send_sem=xs_sem.at[phase, c, k], recv_sem=xr_sem.at[phase, c, k],
                device_id={"gx": to}, device_id_type=pl.DeviceIdType.MESH,
            )
            copy.start()
            copies.append(copy)
        if forward:
            target[:, x_rows(me_x), zs(c)] = source[x_block(me_x), :, zs(c)]
        else:
            target[x_block(me_x), :, zs(c)] = source[:, x_rows(me_x), zs(c)]
        return copies

    def send_y(phase, c, source, target, forward):
        copies = []
        for k in far_first(num_gy):
            to = peer_y(k)
            if forward:
                src, dst = source.at[y_block(to), :, zs(c)], target.at[:, y_rows(me_y), zs(c)]
            else:
                src, dst = source.at[:, y_rows(to), zs(c)], target.at[y_block(me_y), :, zs(c)]
            copy = pltpu.make_async_remote_copy(
                src_ref=src, dst_ref=dst,
                send_sem=ys_sem.at[phase, c, k], recv_sem=yr_sem.at[phase, c, k],
                device_id={"gy": to}, device_id_type=pl.DeviceIdType.MESH,
            )
            copy.start()
            copies.append(copy)
        if forward:
            target[:, y_rows(me_y), zs(c)] = source[y_block(me_y), :, zs(c)]
        else:
            target[y_block(me_y), :, zs(c)] = source[:, y_rows(me_y), zs(c)]
        return copies

    def arrived(copies):
        for copy in copies:
            copy.wait_recv()

    def lines(matrix, source, target, c):
        @pl.loop(0, source.shape[0])
        def _(i):
            target[i, :, zs(c)] = jnp.dot(
                matrix[...], source[i, :, zs(c)],
                precision=highest, preferred_element_type=jnp.float32,
            )

    step = min(8, rows_y)

    def turn_in(source, target, c):
        @pl.loop(0, rows_y // step)
        def _(j):
            y0 = pl.multiple_of(j * step, step)
            target[pl.ds(y0, step), :, zs(c)] = jnp.swapaxes(
                source[:, pl.ds(y0, step), zs(c)], 0, 1
            )

    def turn_out(source, target, c):
        @pl.loop(0, rows_y // step)
        def _(j):
            y0 = pl.multiple_of(j * step, step)
            target[:, pl.ds(y0, step), zs(c)] = jnp.swapaxes(
                source[pl.ds(y0, step), :, zs(c)], 0, 1
            )

    group = min(rows_x, max(1, 256 // rows_y))

    def along_z(source):
        def at(i):
            return pl.ds(i * group, group)

        def product(i):
            flat = source[at(i)].reshape(group * rows_y, count_z)
            result = jnp.dot(
                flat, dmz_ref[...], precision=highest, preferred_element_type=jnp.float32
            )
            return result.reshape(group, rows_y, count_z)

        return at, product

    sent = []
    every = range(chunks)
    fy1, fx1 = [], []
    for c in every:
        turn_in(n_ref, n_t, c)
        fx1.append(send_x(0, c, n_t, lx1, True))
        fy1.append(send_y(0, c, n_ref, ly1, True))
    at, product = along_z(n_ref)

    @pl.loop(0, rows_x // group)
    def _(i):
        gz[at(i)] = product(i)

    by1, bx1 = [], []
    for c in every:
        arrived(fy1[c])
        lines(dmy_ref, ly1, ry1, c)
        by1.append(send_y(1, c, ry1, gy, False))
    for c in every:
        arrived(fx1[c])
        lines(dmx_ref, lx1, rx1, c)
        bx1.append(send_x(1, c, rx1, gx_t, False))

    acc[...] = jnp.zeros_like(acc)
    part = min(rows_y, 32)
    fx2, fy2 = [], []
    for c in every:
        arrived(by1[c])
        arrived(bx1[c])
        turn_out(gx_t, gx, c)

        @pl.loop(0, rows_x)
        def _(i):
            @pl.loop(0, rows_y // part)
            def _(j):
                where = (i, pl.ds(pl.multiple_of(j * part, part), part), zs(c))
                dens, grad_x, grad_y, grad_z = n_ref[where], gx[where], gy[where], gz[where]
                grad_sq = grad_x * grad_x + grad_y * grad_y + grad_z * grad_z
                value, pull = jax.vjp(xc_energy, dens, grad_sq)
                d_dens, d_grad = pull(jnp.ones_like(value))
                twice = 2.0 * d_grad
                out_ref[where] = d_dens
                gx[where] = twice * grad_x
                gy[where] = twice * grad_y
                gz[where] = twice * grad_z
                acc[...] += value

        turn_in(gx, fx_t, c)
        fx2.append(send_x(2, c, fx_t, lx2, True))
        fy2.append(send_y(2, c, gy, ly2, True))

    energy = jnp.sum(acc[...].reshape(-1, 8, zc), axis=0)
    part_y[me_y] = energy
    energy_copies = []
    for k in range(1, num_gy):
        copy = pltpu.make_async_remote_copy(
            src_ref=part_y.at[me_y], dst_ref=part_y.at[me_y],
            send_sem=es_sem.at[0, k], recv_sem=er_sem.at[0, k],
            device_id={"gy": peer_y(k)}, device_id_type=pl.DeviceIdType.MESH,
        )
        copy.start()
        energy_copies.append(copy)

    at, product = along_z(gz)

    @pl.loop(0, rows_x // group)
    def _(i):
        out_ref[at(i)] = out_ref[at(i)] - product(i)

    arrived(energy_copies)
    sent.append(energy_copies)
    tot_y[...] = jnp.sum(part_y[...], axis=0)
    part_x[me_x] = tot_y[...]
    energy_copies = []
    for k in range(1, num_gx):
        copy = pltpu.make_async_remote_copy(
            src_ref=tot_y, dst_ref=part_x.at[me_x],
            send_sem=es_sem.at[1, k], recv_sem=er_sem.at[1, k],
            device_id={"gx": peer_x(k)}, device_id_type=pl.DeviceIdType.MESH,
        )
        copy.start()
        energy_copies.append(copy)

    bx2, by2 = [], []
    for c in every:
        arrived(fy2[c])
        lines(dmy_ref, ly2, ry2, c)
        by2.append(send_y(3, c, ry2, dy, False))
        arrived(fx2[c])
        lines(dmx_ref, lx2, rx2, c)
        bx2.append(send_x(3, c, rx2, dx_t, False))

    arrived(energy_copies)
    sent.append(energy_copies)
    energy_ref[...] = jnp.sum(part_x[...], axis=0)

    for c in every:
        arrived(by2[c])
        arrived(bx2[c])

        @pl.loop(0, rows_y // step)
        def _(j):
            y0 = pl.multiple_of(j * step, step)
            where = (slice(None), pl.ds(y0, step), zs(c))
            turned = jnp.swapaxes(dx_t[pl.ds(y0, step), :, zs(c)], 0, 1)
            out_ref[where] = out_ref[where] - (dy[where] + turned)

    for copies in sent + fx1 + fy1 + bx1 + by1 + fx2 + fy2 + bx2 + by2:
        for copy in copies:
            copy.wait_send()


def body(num_gx, num_gy, density):
    rows_x, rows_y, count_z = density.shape
    count_x = rows_x * num_gx
    count_y = rows_y * num_gy
    zc = 128 if count_z % 128 == 0 else count_z
    chunks = count_z // zc
    block_y = rows_y // num_gx
    block_x = rows_x // num_gy
    straight = (rows_x, rows_y, count_z)
    turned = (rows_y, rows_x, count_z)
    lines_x = (block_y, count_x, count_z)
    lines_y = (block_x, count_y, count_z)
    shapes = [
        turned, lines_x, lines_x, turned, straight,
        lines_y, lines_y, straight, straight,
        turned, lines_x, lines_x, turned,
        lines_y, lines_y, straight,
        (min(rows_y, 32), zc), (num_gy, 8, zc), (8, zc), (num_gx, 8, zc),
    ]
    vmem = pl.BlockSpec(memory_space=pltpu.VMEM)
    potential, partial = pl.pallas_call(
        functools.partial(kernel, num_gx, num_gy, zc),
        out_shape=(
            jax.ShapeDtypeStruct(straight, jnp.float32),
            jax.ShapeDtypeStruct((8, zc), jnp.float32),
        ),
        in_specs=[vmem] * 4,
        out_specs=(vmem, vmem),
        scratch_shapes=[pltpu.VMEM(shape, jnp.float32) for shape in shapes]
        + [
            pltpu.SemaphoreType.DMA((4, chunks, num_gx)),
            pltpu.SemaphoreType.DMA((4, chunks, num_gx)),
            pltpu.SemaphoreType.DMA((4, chunks, num_gy)),
            pltpu.SemaphoreType.DMA((4, chunks, num_gy)),
            pltpu.SemaphoreType.DMA((2, num_gx)),
            pltpu.SemaphoreType.DMA((2, num_gx)),
        ],
        compiler_params=pltpu.CompilerParams(
            collective_id=0, has_side_effects=True, vmem_limit_bytes=60 * 2**20
        ),
    )(
        density,
        jnp.asarray(deriv_matrix(count_x)),
        jnp.asarray(deriv_matrix(count_y)),
        jnp.asarray(deriv_matrix(count_z).T.copy()),
    )
    return (potential, jnp.sum(partial) / float(count_x * count_y * count_z))


def solution(mesh):
    in_specs = (P("gx", "gy", None),)
    out_specs = (P("gx", "gy", None), P())
    run = functools.partial(body, mesh.shape["gx"], mesh.shape["gy"])
    return jax.shard_map(run, mesh=mesh, in_specs=in_specs, out_specs=out_specs, check_vma=False)
```

```python
import functools
import math

import jax
import jax.numpy as jnp
import numpy as np
from jax import lax
from jax.experimental import pallas as pl
from jax.experimental.pallas import tpu as pltpu
from jax.sharding import PartitionSpec as P

spacing = 1.0
highest = lax.Precision.HIGHEST
pbe_kappa = 0.804
pbe_mu = 0.2195149727645171
pbe_beta = 0.06672455060314922
pbe_gamma = 0.031090690869654894
pw_coef = 0.0310907
pw_alpha = 0.2137
pw_first = 7.5957
pw_second = 3.5876
pw_third = 1.6382
pw_fourth = 0.49294


def xc_energy(electrons, grad_sq):
    third = jnp.exp(jnp.log(electrons) * (1.0 / 3.0))
    k_fermi = (3.0 * math.pi**2) ** (1.0 / 3.0) * third
    exch_unif = -0.75 / math.pi * k_fermi
    inv_sq = grad_sq / (4.0 * k_fermi * electrons * electrons)
    s_square = inv_sq / k_fermi
    enhance = 1.0 + pbe_kappa - pbe_kappa / (1.0 + (pbe_mu / pbe_kappa) * s_square)
    wigner = (3.0 / (4.0 * math.pi)) ** (1.0 / 3.0) / third
    root_rs = jnp.sqrt(wigner)
    series = (
        2.0
        * pw_coef
        * root_rs
        * (pw_first + root_rs * (pw_second + root_rs * (pw_third + root_rs * pw_fourth)))
    )
    corr_unif = -2.0 * pw_coef * (1.0 + pw_alpha * wigner) * jnp.log(1.0 + 1.0 / series)
    t_square = inv_sq * (math.pi / 4.0)
    factor = (pbe_beta / pbe_gamma) / (jnp.exp(corr_unif * (-1.0 / pbe_gamma)) - 1.0)
    scaled = factor * t_square
    gradient_term = pbe_gamma * jnp.log(
        1.0 + (pbe_beta / pbe_gamma) * t_square * (1.0 + scaled) / (1.0 + scaled + scaled * scaled)
    )
    return electrons * (exch_unif * enhance + corr_unif + gradient_term)


def deriv_matrix(count):
    positions = np.arange(count)
    signed = np.where(positions < count // 2, positions, positions - count)
    signed = np.where(positions == count // 2, 0, signed)
    waves = signed * (2.0 * math.pi / (count * spacing))
    phase = (positions[:, None] * positions[None, :] % count) * (2.0 * math.pi / count)
    cosine, sine = np.cos(phase), np.sin(phase)
    first = (cosine.T * waves[None, :]) @ sine
    second = (sine.T * waves[None, :]) @ cosine
    return ((first - second) / count).astype(np.float32)


def far_first(count):
    return sorted(range(1, count), key=lambda k: abs(2 * k - count))


def kernel(
    num_gx, num_gy, zc,
    n_hbm, dmx_hbm, dmy_hbm, dmz_hbm,
    out_ref, energy_ref,
    n_ref, dmx_ref, dmy_ref, dmz_ref,
    n_t, lx1, rx1, gx_t, gx, ly1, ry1, gy, gz, fx_t, lx2, rx2, dx_t, ly2, ry2, dy,
    acc, part_y, tot_y, part_x,
    xs_sem, xr_sem, ys_sem, yr_sem, es_sem, er_sem, in_sem,
):
    rows_x, rows_y, count_z = n_ref.shape
    block_y = rows_y // num_gx
    block_x = rows_x // num_gy
    count_x = rows_x * num_gx
    count_y = rows_y * num_gy
    chunks = count_z // zc
    me_x = lax.axis_index("gx")
    me_y = lax.axis_index("gy")

    def peer_x(k):
        return lax.rem(me_x + k, num_gx)

    def peer_y(k):
        return lax.rem(me_y + k, num_gy)

    def zs(c):
        return pl.ds(c * zc, zc)

    def x_block(i):
        return pl.ds(i * block_y, block_y)

    def x_rows(i):
        return pl.ds(pl.multiple_of(i * rows_x, rows_x), rows_x)

    def y_block(i):
        return pl.ds(i * block_x, block_x)

    def y_rows(i):
        return pl.ds(pl.multiple_of(i * rows_y, rows_y), rows_y)

    loads = [
        pltpu.make_async_copy(n_hbm.at[:, :, zs(c)], n_ref.at[:, :, zs(c)], in_sem.at[c])
        for c in range(chunks)
    ]
    pairs = ((dmz_hbm, dmz_ref), (dmy_hbm, dmy_ref), (dmx_hbm, dmx_ref))
    tables = [
        pltpu.make_async_copy(source, target, in_sem.at[chunks + place])
        for place, (source, target) in enumerate(pairs)
    ]
    for copy in loads + tables:
        copy.start()
    barrier = pltpu.get_barrier_semaphore()
    for k in range(1, num_gx):
        pl.semaphore_signal(
            barrier, inc=1, device_id={"gx": peer_x(k)}, device_id_type=pl.DeviceIdType.MESH
        )
    for k in range(1, num_gy):
        pl.semaphore_signal(
            barrier, inc=1, device_id={"gy": peer_y(k)}, device_id_type=pl.DeviceIdType.MESH
        )
    def send_x(phase, c, source, target, forward):
        copies = []
        for k in far_first(num_gx):
            to = peer_x(k)
            if forward:
                src, dst = source.at[x_block(to), :, zs(c)], target.at[:, x_rows(me_x), zs(c)]
            else:
                src, dst = source.at[:, x_rows(to), zs(c)], target.at[x_block(me_x), :, zs(c)]
            copy = pltpu.make_async_remote_copy(
                src_ref=src, dst_ref=dst,
                send_sem=xs_sem.at[phase, c, k], recv_sem=xr_sem.at[phase, c, k],
                device_id={"gx": to}, device_id_type=pl.DeviceIdType.MESH,
            )
            copy.start()
            copies.append(copy)
        if forward:
            target[:, x_rows(me_x), zs(c)] = source[x_block(me_x), :, zs(c)]
        else:
            target[x_block(me_x), :, zs(c)] = source[:, x_rows(me_x), zs(c)]
        return copies

    def send_y(phase, c, source, target, forward):
        copies = []
        for k in far_first(num_gy):
            to = peer_y(k)
            if forward:
                src, dst = source.at[y_block(to), :, zs(c)], target.at[:, y_rows(me_y), zs(c)]
            else:
                src, dst = source.at[:, y_rows(to), zs(c)], target.at[y_block(me_y), :, zs(c)]
            copy = pltpu.make_async_remote_copy(
                src_ref=src, dst_ref=dst,
                send_sem=ys_sem.at[phase, c, k], recv_sem=yr_sem.at[phase, c, k],
                device_id={"gy": to}, device_id_type=pl.DeviceIdType.MESH,
            )
            copy.start()
            copies.append(copy)
        if forward:
            target[:, y_rows(me_y), zs(c)] = source[y_block(me_y), :, zs(c)]
        else:
            target[y_block(me_y), :, zs(c)] = source[:, y_rows(me_y), zs(c)]
        return copies

    def arrived(copies):
        for copy in copies:
            copy.wait_recv()

    def lines(matrix, source, target, c):
        @pl.loop(0, source.shape[0])
        def _(i):
            target[i, :, zs(c)] = jnp.dot(
                matrix[...], source[i, :, zs(c)],
                precision=highest, preferred_element_type=jnp.float32,
            )

    step = min(8, rows_y)

    def turn_in(source, target, c):
        @pl.loop(0, rows_y // step)
        def _(j):
            y0 = pl.multiple_of(j * step, step)
            target[pl.ds(y0, step), :, zs(c)] = jnp.swapaxes(
                source[:, pl.ds(y0, step), zs(c)], 0, 1
            )

    def turn_out(source, target, c):
        @pl.loop(0, rows_y // step)
        def _(j):
            y0 = pl.multiple_of(j * step, step)
            target[:, pl.ds(y0, step), zs(c)] = jnp.swapaxes(
                source[pl.ds(y0, step), :, zs(c)], 0, 1
            )

    group = min(rows_x, max(1, 256 // rows_y))

    def along_z(source):
        def at(i):
            return pl.ds(i * group, group)

        def product(i):
            flat = source[at(i)].reshape(group * rows_y, count_z)
            result = jnp.dot(
                flat, dmz_ref[...], precision=highest, preferred_element_type=jnp.float32
            )
            return result.reshape(group, rows_y, count_z)

        return at, product

    sent = []
    every = range(chunks)
    fy1, fx1 = [], []
    for c in every:
        loads[c].wait()
        turn_in(n_ref, n_t, c)
        if c == 0:
            pl.semaphore_wait(barrier, num_gx + num_gy - 2)
        fx1.append(send_x(0, c, n_t, lx1, True))
        fy1.append(send_y(0, c, n_ref, ly1, True))
    for copy in tables:
        copy.wait()
    at, product = along_z(n_ref)

    @pl.loop(0, rows_x // group)
    def _(i):
        gz[at(i)] = product(i)

    by1, bx1 = [], []
    for c in every:
        arrived(fy1[c])
        lines(dmy_ref, ly1, ry1, c)
        by1.append(send_y(1, c, ry1, gy, False))
    for c in every:
        arrived(fx1[c])
        lines(dmx_ref, lx1, rx1, c)
        bx1.append(send_x(1, c, rx1, gx_t, False))

    acc[...] = jnp.zeros_like(acc)
    part = min(rows_y, 32)
    fx2, fy2 = [], []
    for c in every:
        arrived(by1[c])
        arrived(bx1[c])
        turn_out(gx_t, gx, c)

        @pl.loop(0, rows_x)
        def _(i):
            @pl.loop(0, rows_y // part)
            def _(j):
                where = (i, pl.ds(pl.multiple_of(j * part, part), part), zs(c))
                dens, grad_x, grad_y, grad_z = n_ref[where], gx[where], gy[where], gz[where]
                grad_sq = grad_x * grad_x + grad_y * grad_y + grad_z * grad_z
                value, pull = jax.vjp(xc_energy, dens, grad_sq)
                d_dens, d_grad = pull(jnp.ones_like(value))
                twice = 2.0 * d_grad
                out_ref[where] = d_dens
                gx[where] = twice * grad_x
                gy[where] = twice * grad_y
                gz[where] = twice * grad_z
                acc[...] += value

        turn_in(gx, fx_t, c)
        fx2.append(send_x(2, c, fx_t, lx2, True))
        fy2.append(send_y(2, c, gy, ly2, True))

    energy = jnp.sum(acc[...].reshape(-1, 8, zc), axis=0)
    part_y[me_y] = energy
    energy_copies = []
    for k in range(1, num_gy):
        copy = pltpu.make_async_remote_copy(
            src_ref=part_y.at[me_y], dst_ref=part_y.at[me_y],
            send_sem=es_sem.at[0, k], recv_sem=er_sem.at[0, k],
            device_id={"gy": peer_y(k)}, device_id_type=pl.DeviceIdType.MESH,
        )
        copy.start()
        energy_copies.append(copy)

    at, product = along_z(gz)

    @pl.loop(0, rows_x // group)
    def _(i):
        out_ref[at(i)] = out_ref[at(i)] - product(i)

    arrived(energy_copies)
    sent.append(energy_copies)
    tot_y[...] = jnp.sum(part_y[...], axis=0)
    part_x[me_x] = tot_y[...]
    energy_copies = []
    for k in range(1, num_gx):
        copy = pltpu.make_async_remote_copy(
            src_ref=tot_y, dst_ref=part_x.at[me_x],
            send_sem=es_sem.at[1, k], recv_sem=er_sem.at[1, k],
            device_id={"gx": peer_x(k)}, device_id_type=pl.DeviceIdType.MESH,
        )
        copy.start()
        energy_copies.append(copy)

    bx2, by2 = [], []
    for c in every:
        arrived(fy2[c])
        lines(dmy_ref, ly2, ry2, c)
        by2.append(send_y(3, c, ry2, dy, False))
        arrived(fx2[c])
        lines(dmx_ref, lx2, rx2, c)
        bx2.append(send_x(3, c, rx2, dx_t, False))

    arrived(energy_copies)
    sent.append(energy_copies)
    cells = float(count_x * count_y * count_z)
    total = jnp.sum(part_x[...], axis=0)
    energy_ref[...] = jnp.sum(total, axis=(0, 1), keepdims=True) * (1.0 / cells)

    for c in every:
        arrived(by2[c])
        arrived(bx2[c])

        @pl.loop(0, rows_y // step)
        def _(j):
            y0 = pl.multiple_of(j * step, step)
            where = (slice(None), pl.ds(y0, step), zs(c))
            turned = jnp.swapaxes(dx_t[pl.ds(y0, step), :, zs(c)], 0, 1)
            out_ref[where] = out_ref[where] - (dy[where] + turned)

    for copies in sent + fx1 + fy1 + bx1 + by1 + fx2 + fy2 + bx2 + by2:
        for copy in copies:
            copy.wait_send()


def body(num_gx, num_gy, density):
    rows_x, rows_y, count_z = density.shape
    count_x = rows_x * num_gx
    count_y = rows_y * num_gy
    zc = 128 if count_z % 128 == 0 else count_z
    chunks = count_z // zc
    block_y = rows_y // num_gx
    block_x = rows_x // num_gy
    straight = (rows_x, rows_y, count_z)
    turned = (rows_y, rows_x, count_z)
    lines_x = (block_y, count_x, count_z)
    lines_y = (block_x, count_y, count_z)
    shapes = [
        straight, (count_x, count_x), (count_y, count_y), (count_z, count_z),
        turned, lines_x, lines_x, turned, straight,
        lines_y, lines_y, straight, straight,
        turned, lines_x, lines_x, turned,
        lines_y, lines_y, straight,
        (min(rows_y, 32), zc), (num_gy, 8, zc), (8, zc), (num_gx, 8, zc),
    ]
    vmem = pl.BlockSpec(memory_space=pltpu.VMEM)
    potential, partial = pl.pallas_call(
        functools.partial(kernel, num_gx, num_gy, zc),
        out_shape=(
            pltpu.VMEM(straight, jnp.float32),
            jax.ShapeDtypeStruct((1, 1), jnp.float32),
        ),
        in_specs=[pl.BlockSpec(memory_space=pltpu.HBM)] * 4,
        out_specs=(vmem, vmem),
        scratch_shapes=[pltpu.VMEM(shape, jnp.float32) for shape in shapes]
        + [
            pltpu.SemaphoreType.DMA((4, chunks, num_gx)),
            pltpu.SemaphoreType.DMA((4, chunks, num_gx)),
            pltpu.SemaphoreType.DMA((4, chunks, num_gy)),
            pltpu.SemaphoreType.DMA((4, chunks, num_gy)),
            pltpu.SemaphoreType.DMA((2, num_gx)),
            pltpu.SemaphoreType.DMA((2, num_gx)),
            pltpu.SemaphoreType.DMA((chunks + 3,)),
        ],
        compiler_params=pltpu.CompilerParams(
            collective_id=0, has_side_effects=True, vmem_limit_bytes=67043328 - 4 * density.size - 2**16
        ),
    )(
        density,
        jnp.asarray(deriv_matrix(count_x)),
        jnp.asarray(deriv_matrix(count_y)),
        jnp.asarray(deriv_matrix(count_z).T.copy()),
    )
    return (potential, partial.reshape(()))


def solution(mesh):
    in_specs = (P("gx", "gy", None),)
    out_specs = (P("gx", "gy", None), P())
    run = functools.partial(body, mesh.shape["gx"], mesh.shape["gy"])
    return jax.shard_map(run, mesh=mesh, in_specs=in_specs, out_specs=out_specs, check_vma=False)
```

```python
import functools
import math

import jax
import jax.numpy as jnp
import numpy as np
from jax import lax
from jax.experimental import pallas as pl
from jax.experimental.pallas import tpu as pltpu
from jax.sharding import PartitionSpec as P

spacing = 1.0
highest = lax.Precision.HIGHEST
pbe_kappa = 0.804
pbe_mu = 0.2195149727645171
pbe_beta = 0.06672455060314922
pbe_gamma = 0.031090690869654894
pw_coef = 0.0310907
pw_alpha = 0.2137
pw_first = 7.5957
pw_second = 3.5876
pw_third = 1.6382
pw_fourth = 0.49294


def xc_energy(electrons, grad_sq):
    third = jnp.exp(jnp.log(electrons) * (1.0 / 3.0))
    k_fermi = (3.0 * math.pi**2) ** (1.0 / 3.0) * third
    exch_unif = -0.75 / math.pi * k_fermi
    inv_sq = grad_sq / (4.0 * k_fermi * electrons * electrons)
    s_square = inv_sq / k_fermi
    enhance = 1.0 + pbe_kappa - pbe_kappa / (1.0 + (pbe_mu / pbe_kappa) * s_square)
    wigner = (3.0 / (4.0 * math.pi)) ** (1.0 / 3.0) / third
    root_rs = jnp.sqrt(wigner)
    series = (
        2.0
        * pw_coef
        * root_rs
        * (pw_first + root_rs * (pw_second + root_rs * (pw_third + root_rs * pw_fourth)))
    )
    corr_unif = -2.0 * pw_coef * (1.0 + pw_alpha * wigner) * jnp.log(1.0 + 1.0 / series)
    t_square = inv_sq * (math.pi / 4.0)
    factor = (pbe_beta / pbe_gamma) / (jnp.exp(corr_unif * (-1.0 / pbe_gamma)) - 1.0)
    scaled = factor * t_square
    gradient_term = pbe_gamma * jnp.log(
        1.0 + (pbe_beta / pbe_gamma) * t_square * (1.0 + scaled) / (1.0 + scaled + scaled * scaled)
    )
    return electrons * (exch_unif * enhance + corr_unif + gradient_term)


def deriv_matrix(count):
    positions = np.arange(count)
    signed = np.where(positions < count // 2, positions, positions - count)
    signed = np.where(positions == count // 2, 0, signed)
    waves = signed * (2.0 * math.pi / (count * spacing))
    phase = (positions[:, None] * positions[None, :] % count) * (2.0 * math.pi / count)
    cosine, sine = np.cos(phase), np.sin(phase)
    first = (cosine.T * waves[None, :]) @ sine
    second = (sine.T * waves[None, :]) @ cosine
    return ((first - second) / count).astype(np.float32)


def far_first(count):
    return sorted(range(1, count), key=lambda k: abs(2 * k - count))


def kernel(
    num_gx, num_gy, zc,
    n_hbm, dmx_hbm, dmy_hbm, dmz_hbm,
    out_ref, energy_ref,
    n_ref, dmx_ref, dmy_ref, dmz_ref,
    n_t, lx1, rx1, gx_t, gx, ly1, ry1, gy, gz, fx_t, lx2, rx2, dx_t, ly2, ry2, dy,
    acc, part_y, tot_y, part_x,
    xs_sem, xr_sem, ys_sem, yr_sem, es_sem, er_sem, in_sem,
):
    rows_x, rows_y, count_z = n_ref.shape
    block_y = rows_y // num_gx
    block_x = rows_x // num_gy
    count_x = rows_x * num_gx
    count_y = rows_y * num_gy
    chunks = count_z // zc
    me_x = lax.axis_index("gx")
    me_y = lax.axis_index("gy")

    def peer_x(k):
        return lax.rem(me_x + k, num_gx)

    def peer_y(k):
        return lax.rem(me_y + k, num_gy)

    def zs(c):
        return pl.ds(c * zc, zc)

    def x_block(i):
        return pl.ds(i * block_y, block_y)

    def x_rows(i):
        return pl.ds(pl.multiple_of(i * rows_x, rows_x), rows_x)

    def y_block(i):
        return pl.ds(i * block_x, block_x)

    def y_rows(i):
        return pl.ds(pl.multiple_of(i * rows_y, rows_y), rows_y)

    loads = [
        pltpu.make_async_copy(n_hbm.at[:, :, zs(c)], n_ref.at[:, :, zs(c)], in_sem.at[c])
        for c in range(chunks)
    ]
    pairs = ((dmz_hbm, dmz_ref), (dmy_hbm, dmy_ref), (dmx_hbm, dmx_ref))
    tables = [
        pltpu.make_async_copy(source, target, in_sem.at[chunks + place])
        for place, (source, target) in enumerate(pairs)
    ]
    for copy in loads + tables:
        copy.start()
    barrier = pltpu.get_barrier_semaphore()
    for k in range(1, num_gx):
        pl.semaphore_signal(
            barrier, inc=1, device_id={"gx": peer_x(k)}, device_id_type=pl.DeviceIdType.MESH
        )
    for k in range(1, num_gy):
        pl.semaphore_signal(
            barrier, inc=1, device_id={"gy": peer_y(k)}, device_id_type=pl.DeviceIdType.MESH
        )
    def send_x(phase, c, source, target, forward, prepare=None):
        copies = []
        for k in far_first(num_gx):
            to = peer_x(k)
            if prepare is not None:
                prepare(to)
            if forward:
                src, dst = source.at[x_block(to), :, zs(c)], target.at[:, x_rows(me_x), zs(c)]
            else:
                src, dst = source.at[:, x_rows(to), zs(c)], target.at[x_block(me_x), :, zs(c)]
            copy = pltpu.make_async_remote_copy(
                src_ref=src, dst_ref=dst,
                send_sem=xs_sem.at[phase, c, k], recv_sem=xr_sem.at[phase, c, k],
                device_id={"gx": to}, device_id_type=pl.DeviceIdType.MESH,
            )
            copy.start()
            copies.append(copy)
        if forward:
            target[:, x_rows(me_x), zs(c)] = source[x_block(me_x), :, zs(c)]
        else:
            target[x_block(me_x), :, zs(c)] = source[:, x_rows(me_x), zs(c)]
        return copies

    def send_y(phase, c, source, target, forward):
        copies = []
        for k in far_first(num_gy):
            to = peer_y(k)
            if forward:
                src, dst = source.at[y_block(to), :, zs(c)], target.at[:, y_rows(me_y), zs(c)]
            else:
                src, dst = source.at[:, y_rows(to), zs(c)], target.at[y_block(me_y), :, zs(c)]
            copy = pltpu.make_async_remote_copy(
                src_ref=src, dst_ref=dst,
                send_sem=ys_sem.at[phase, c, k], recv_sem=yr_sem.at[phase, c, k],
                device_id={"gy": to}, device_id_type=pl.DeviceIdType.MESH,
            )
            copy.start()
            copies.append(copy)
        if forward:
            target[:, y_rows(me_y), zs(c)] = source[y_block(me_y), :, zs(c)]
        else:
            target[y_block(me_y), :, zs(c)] = source[:, y_rows(me_y), zs(c)]
        return copies

    def arrived(copies):
        for copy in copies:
            copy.wait_recv()

    def lines(matrix, source, target, c):
        @pl.loop(0, source.shape[0])
        def _(i):
            target[i, :, zs(c)] = jnp.dot(
                matrix[...], source[i, :, zs(c)],
                precision=highest, preferred_element_type=jnp.float32,
            )

    step = min(8, rows_y)

    def turn_in(source, target, c):
        @pl.loop(0, rows_y // step)
        def _(j):
            y0 = pl.multiple_of(j * step, step)
            target[pl.ds(y0, step), :, zs(c)] = jnp.swapaxes(
                source[:, pl.ds(y0, step), zs(c)], 0, 1
            )

    def turn_out(source, target, c):
        @pl.loop(0, rows_y // step)
        def _(j):
            y0 = pl.multiple_of(j * step, step)
            target[:, pl.ds(y0, step), zs(c)] = jnp.swapaxes(
                source[pl.ds(y0, step), :, zs(c)], 0, 1
            )

    group = min(rows_x, max(1, 256 // rows_y))

    def along_z(source):
        def at(i):
            return pl.ds(i * group, group)

        def product(i):
            flat = source[at(i)].reshape(group * rows_y, count_z)
            result = jnp.dot(
                flat, dmz_ref[...], precision=highest, preferred_element_type=jnp.float32
            )
            return result.reshape(group, rows_y, count_z)

        return at, product

    sent = []
    every = range(chunks)
    fy1, fx1 = [], []
    for c in every:
        loads[c].wait()
        prepare = None
        if block_y == step:

            def prepare(to, c=c):
                y0 = pl.multiple_of(to * step, step)
                n_t[pl.ds(y0, step), :, zs(c)] = jnp.swapaxes(
                    n_ref[:, pl.ds(y0, step), zs(c)], 0, 1
                )

            prepare(me_x)
        else:
            turn_in(n_ref, n_t, c)
        if c == 0:
            pl.semaphore_wait(barrier, num_gx + num_gy - 2)
        fx1.append(send_x(0, c, n_t, lx1, True, prepare))
        fy1.append(send_y(0, c, n_ref, ly1, True))
    for copy in tables:
        copy.wait()
    at, product = along_z(n_ref)

    @pl.loop(0, rows_x // group)
    def _(i):
        gz[at(i)] = product(i)

    by1, bx1 = [], []
    for c in every:
        arrived(fy1[c])
        lines(dmy_ref, ly1, ry1, c)
        by1.append(send_y(1, c, ry1, gy, False))
    for c in every:
        arrived(fx1[c])
        lines(dmx_ref, lx1, rx1, c)
        bx1.append(send_x(1, c, rx1, gx_t, False))

    acc[...] = jnp.zeros_like(acc)
    part = min(rows_y, 32)
    fx2, fy2 = [], []
    for c in every:
        arrived(by1[c])
        arrived(bx1[c])
        turn_out(gx_t, gx, c)

        @pl.loop(0, rows_x)
        def _(i):
            @pl.loop(0, rows_y // part)
            def _(j):
                where = (i, pl.ds(pl.multiple_of(j * part, part), part), zs(c))
                dens, grad_x, grad_y, grad_z = n_ref[where], gx[where], gy[where], gz[where]
                grad_sq = grad_x * grad_x + grad_y * grad_y + grad_z * grad_z
                value, pull = jax.vjp(xc_energy, dens, grad_sq)
                d_dens, d_grad = pull(jnp.ones_like(value))
                twice = 2.0 * d_grad
                out_ref[where] = d_dens
                gx[where] = twice * grad_x
                gy[where] = twice * grad_y
                gz[where] = twice * grad_z
                acc[...] += value

        turn_in(gx, fx_t, c)
        fx2.append(send_x(2, c, fx_t, lx2, True))
        fy2.append(send_y(2, c, gy, ly2, True))

    energy = jnp.sum(acc[...].reshape(-1, 8, zc), axis=0)
    part_y[me_y] = energy
    energy_copies = []
    for k in range(1, num_gy):
        copy = pltpu.make_async_remote_copy(
            src_ref=part_y.at[me_y], dst_ref=part_y.at[me_y],
            send_sem=es_sem.at[0, k], recv_sem=er_sem.at[0, k],
            device_id={"gy": peer_y(k)}, device_id_type=pl.DeviceIdType.MESH,
        )
        copy.start()
        energy_copies.append(copy)

    at, product = along_z(gz)

    @pl.loop(0, rows_x // group)
    def _(i):
        out_ref[at(i)] = out_ref[at(i)] - product(i)

    arrived(energy_copies)
    sent.append(energy_copies)
    tot_y[...] = jnp.sum(part_y[...], axis=0)
    part_x[me_x] = tot_y[...]
    energy_copies = []
    for k in range(1, num_gx):
        copy = pltpu.make_async_remote_copy(
            src_ref=tot_y, dst_ref=part_x.at[me_x],
            send_sem=es_sem.at[1, k], recv_sem=er_sem.at[1, k],
            device_id={"gx": peer_x(k)}, device_id_type=pl.DeviceIdType.MESH,
        )
        copy.start()
        energy_copies.append(copy)

    bx2, by2 = [], []
    for c in every:
        arrived(fy2[c])
        lines(dmy_ref, ly2, ry2, c)
        by2.append(send_y(3, c, ry2, dy, False))
        arrived(fx2[c])
        lines(dmx_ref, lx2, rx2, c)
        bx2.append(send_x(3, c, rx2, dx_t, False))

    arrived(energy_copies)
    sent.append(energy_copies)
    cells = float(count_x * count_y * count_z)
    total = jnp.sum(part_x[...], axis=0)
    energy_ref[...] = jnp.sum(total, axis=(0, 1), keepdims=True) * (1.0 / cells)

    for c in every:
        arrived(by2[c])
        arrived(bx2[c])

        @pl.loop(0, rows_y // step)
        def _(j):
            y0 = pl.multiple_of(j * step, step)
            where = (slice(None), pl.ds(y0, step), zs(c))
            turned = jnp.swapaxes(dx_t[pl.ds(y0, step), :, zs(c)], 0, 1)
            out_ref[where] = out_ref[where] - (dy[where] + turned)

    for copies in sent + fx1 + fy1 + bx1 + by1 + fx2 + fy2 + bx2 + by2:
        for copy in copies:
            copy.wait_send()


def body(num_gx, num_gy, density):
    rows_x, rows_y, count_z = density.shape
    count_x = rows_x * num_gx
    count_y = rows_y * num_gy
    zc = 128 if count_z % 128 == 0 else count_z
    chunks = count_z // zc
    block_y = rows_y // num_gx
    block_x = rows_x // num_gy
    straight = (rows_x, rows_y, count_z)
    turned = (rows_y, rows_x, count_z)
    lines_x = (block_y, count_x, count_z)
    lines_y = (block_x, count_y, count_z)
    shapes = [
        straight, (count_x, count_x), (count_y, count_y), (count_z, count_z),
        turned, lines_x, lines_x, turned, straight,
        lines_y, lines_y, straight, straight,
        turned, lines_x, lines_x, turned,
        lines_y, lines_y, straight,
        (min(rows_y, 32), zc), (num_gy, 8, zc), (8, zc), (num_gx, 8, zc),
    ]
    vmem = pl.BlockSpec(memory_space=pltpu.VMEM)
    potential, partial = pl.pallas_call(
        functools.partial(kernel, num_gx, num_gy, zc),
        out_shape=(
            pltpu.VMEM(straight, jnp.float32),
            jax.ShapeDtypeStruct((1, 1), jnp.float32),
        ),
        in_specs=[pl.BlockSpec(memory_space=pltpu.HBM)] * 4,
        out_specs=(vmem, vmem),
        scratch_shapes=[pltpu.VMEM(shape, jnp.float32) for shape in shapes]
        + [
            pltpu.SemaphoreType.DMA((4, chunks, num_gx)),
            pltpu.SemaphoreType.DMA((4, chunks, num_gx)),
            pltpu.SemaphoreType.DMA((4, chunks, num_gy)),
            pltpu.SemaphoreType.DMA((4, chunks, num_gy)),
            pltpu.SemaphoreType.DMA((2, num_gx)),
            pltpu.SemaphoreType.DMA((2, num_gx)),
            pltpu.SemaphoreType.DMA((chunks + 3,)),
        ],
        compiler_params=pltpu.CompilerParams(
            collective_id=0, has_side_effects=True, vmem_limit_bytes=67043328 - 4 * density.size - 2**16
        ),
    )(
        density,
        jnp.asarray(deriv_matrix(count_x)),
        jnp.asarray(deriv_matrix(count_y)),
        jnp.asarray(deriv_matrix(count_z).T.copy()),
    )
    return (potential, partial.reshape(()))


def solution(mesh):
    in_specs = (P("gx", "gy", None),)
    out_specs = (P("gx", "gy", None), P())
    run = functools.partial(body, mesh.shape["gx"], mesh.shape["gy"])
    return jax.shard_map(run, mesh=mesh, in_specs=in_specs, out_specs=out_specs, check_vma=False)
```
